32 devices in a mesh: band: 8 (over z, y), mp: 4 (over x, core).
Axes of the slice: x: 2, y: 2, z: 4, core: 2. Of those that a mesh axis runs over, the one named last changes fastest.
Arguments:
- grid_latent: bfloat16 [32768, 512], P('band'), may hold values from -6 to 6
- edge_latent: bfloat16 [49152, 512], P('band'), may hold values from -6 to 6
- mesh_latent: bfloat16 [5120, 512], P('band', 'mp'), may hold values from -6 to 6
- mesh_grad: bfloat16 [5120, 512], P('band', 'mp'), may hold values from -96 to 96
- counts: int32 [5120], P('band'), may hold values from 8 to 64
- request: int32 [8, 7, 128], P('band'), may hold values from -1 to 639, as said below
- edge_sender: int32 [49152], P('band'), may hold values from 0 to 4095, as said below
- edge_slot: int32 [49152], P('band'), may hold values from 0 to 895, as said below
- w_send: bfloat16 [512, 512], P(None, 'mp'), may hold values from -0.25 to 0.25
- w_recv: bfloat16 [512, 512], P(None, 'mp'), may hold values from -0.25 to 0.25
- w_edge: bfloat16 [512, 512], P(None, 'mp'), may hold values from -0.25 to 0.25
- edge_bias: float32 [512], P('mp'), may hold values from -3 to 3
- w_out: bfloat16 [512, 512], P('mp'), may hold values from -0.25 to 0.25
Outputs:
- grid_grad: bfloat16 [32768, 512], P('band', 'mp')
- node_grad: bfloat16 [5120, 512], P('band', 'mp')
The draws below stay inside these ranges and needn't reach their ends.
Inputs may be any that keep to these rules, and one draw needn't show every extreme that they name: request[p, k, c] is a node of patch p, numbered within the patch, wanted by band p + 3 - k, or -1 for an empty slot; where that band lies outside 0 to 7 all slots are -1; otherwise the live slots come first, name distinct nodes and number 1 or more; request[p, 3, c] is live for every c. `edge_sender`: within a band the senders never fall, and each grid point of the band sends one or two edges. edge_slot = k * 128 + c, the patch b + k - 3 of the edge's band b lies in 0 to 7, and request[b + k - 3, k, c] is never -1.
All inputs are finite; a program needn't handle non-finite values.
Results may differ from the reference program's by a relative error of at most 0.015.
Values may be sent and summed in bfloat16 or wider, within the bound.
A program may use at most 64 MiB of HBM per device.

```python
import jax
import jax.numpy as jnp
from jax import lax

LATENT = 512
HIDDEN_SIZE = 512
G_DEV = 4096
EDGE_DEV = 6144
M_DEV = 640
CAPACITY = 128
REACH = 3
SPAN = 7
GRID = 32768
EDGES = 49152
MESH = 5120
N_BAND = 8


def live_counts(key):
    band_index = jnp.arange(N_BAND, dtype=jnp.int32)
    offsets = jnp.arange(SPAN, dtype=jnp.int32)
    patches = band_index[:, None] + offsets[None, :] - REACH
    inside = (patches >= 0) & (patches < N_BAND)
    distance = jnp.abs(offsets - REACH)
    highest = CAPACITY - distance * CAPACITY // (REACH + 1)
    jitter = jax.random.randint(key, (N_BAND, SPAN), 0, CAPACITY // 8 + 1)
    lowered = jnp.clip(highest[None, :] - jitter, 1, CAPACITY)
    lowered = jnp.where((distance == 0)[None, :], CAPACITY, lowered)
    return jnp.where(inside, lowered, 0).astype(jnp.int32)


def draw_request(key, part):
    live = live_counts(jax.random.fold_in(key, 7))
    patch_index = jnp.arange(N_BAND, dtype=jnp.int32)
    offsets = jnp.arange(SPAN, dtype=jnp.int32)
    bands = patch_index[:, None] + REACH - offsets[None, :]
    inside = (bands >= 0) & (bands < N_BAND)
    band_clip = jnp.clip(bands, 0, N_BAND - 1)
    live_here = jnp.where(inside, live[band_clip, offsets[None, :]], 0)
    scores = jax.random.randint(jax.random.fold_in(key, 11), (N_BAND, SPAN, M_DEV), 0, 1 << 20)
    scores = scores * M_DEV + jnp.arange(M_DEV, dtype=jnp.int32)
    ordered = jnp.argsort(scores, axis=-1)[:, :, :CAPACITY].astype(jnp.int32)
    column = jnp.arange(CAPACITY, dtype=jnp.int32)
    return jnp.where(column[None, None, :] < live_here[:, :, None], ordered, -1).astype(jnp.int32)


def draw_edge_slot(key, part):
    live = live_counts(jax.random.fold_in(key, 7))
    first_key, second_key = jax.random.split(jax.random.fold_in(key, 13))
    band_index = jnp.arange(N_BAND, dtype=jnp.int32)
    lowest = jnp.maximum(0, REACH - band_index)
    highest = jnp.minimum(SPAN - 1, REACH + N_BAND - 1 - band_index) + 1
    offset = lowest[:, None] + jax.random.randint(first_key, (N_BAND, EDGE_DEV), 0, (highest - lowest)[:, None])
    bounds = jnp.take_along_axis(live, offset, axis=1)
    column = jax.random.randint(second_key, (N_BAND, EDGE_DEV), 0, bounds)
    return (offset * CAPACITY + column).reshape(-1).astype(jnp.int32)


def draw_edge_sender(key, part):
    scores = jax.random.randint(key, (N_BAND, G_DEV), 0, 1 << 18) * G_DEV + jnp.arange(G_DEV, dtype=jnp.int32)
    ranking = jnp.argsort(jnp.argsort(scores, axis=-1), axis=-1)
    repeats = 1 + (ranking < G_DEV // 2).astype(jnp.int32)

    def spread(repeat_row):
        return jnp.repeat(jnp.arange(G_DEV, dtype=jnp.int32), repeat_row, total_repeat_length=EDGE_DEV)
    return jax.vmap(spread)(repeats).reshape(-1).astype(jnp.int32)


def place_ends(entries, stream_key, low, high):
    index_at = [jax.random.randint(jax.random.fold_in(stream_key, axis), (), 0, length) for axis, length in enumerate(entries.shape)]
    widest = entries.shape.index(max(entries.shape))
    neighbour = index_at[:widest] + [(index_at[widest] + 1) % entries.shape[widest]] + index_at[widest + 1:]
    return entries.at[tuple(index_at)].set(low).at[tuple(neighbour)].set(high)


def levels(own_key, extent, shards, low, top_value):
    factor_of = 1.0
    for position, shards_of in shards:
        steps = jax.random.uniform(jax.random.fold_in(jax.random.fold_in(own_key, 6), position), (shards_of,), jnp.float32, low / len(shards), top_value / len(shards))
        factor_of = factor_of * jnp.repeat(jnp.exp(steps), extent[position] // shards_of).reshape((-1,) + (1,) * (len(extent) - 1 - position))
    return factor_of


def normal_values(key, extent, scale, bound, cuts=(), kind=jnp.bfloat16):
    result = jax.random.normal(key, extent, jnp.float32) * scale
    if len(cuts) > 0:
        result = levels(key, extent, cuts, -0.22, 0.18) * result
    return jnp.clip(result, min=-bound, max=bound).astype(kind)


def setup_inputs(seed: int = 0) -> dict:
    splits = jax.random.split(jax.random.key(seed), 14)
    grid_latent = normal_values(splits[0], (GRID, LATENT), 1.0, 6.0, ((0, 8),))
    edge_latent = normal_values(splits[1], (EDGES, LATENT), 1.0, 6.0, ((0, 8),))
    mesh_latent = normal_values(splits[2], (MESH, LATENT), 1.0, 6.0, ((0, 8), (1, 4)))
    mesh_grad = normal_values(splits[3], (MESH, LATENT), 16.0, 96.0, ((0, 8), (1, 4)))
    counts = place_ends(jax.random.randint(splits[4], (MESH,), 8, 65), jax.random.fold_in(splits[4], 1), 8, 64).astype(jnp.int32)
    request = draw_request(jax.random.fold_in(splits[13], 71), 0)
    edge_sender = draw_edge_sender(jax.random.fold_in(splits[13], 71), 0)
    edge_slot = draw_edge_slot(jax.random.fold_in(splits[13], 71), 0)
    w_send = normal_values(splits[8], (LATENT, HIDDEN_SIZE), LATENT ** -0.5, 0.25, ((1, 4),))
    w_recv = normal_values(splits[9], (LATENT, HIDDEN_SIZE), LATENT ** -0.5, 0.25, ((1, 4),))
    w_edge = normal_values(splits[10], (LATENT, HIDDEN_SIZE), LATENT ** -0.5, 0.25, ((1, 4),))
    edge_bias = normal_values(splits[11], (HIDDEN_SIZE,), 0.5, 3.0, ((0, 4),), jnp.float32)
    w_out = normal_values(splits[12], (HIDDEN_SIZE, LATENT), HIDDEN_SIZE ** -0.5, 0.25, ((0, 4),))
    return {"grid_latent": grid_latent, "edge_latent": edge_latent, "mesh_latent": mesh_latent, "mesh_grad": mesh_grad, "counts": counts, "request": request, "edge_sender": edge_sender, "edge_slot": edge_slot, "w_send": w_send, "w_recv": w_recv, "w_edge": w_edge, "edge_bias": edge_bias, "w_out": w_out}


def silu_slope(pre_act):
    sigmoid_value = jax.nn.sigmoid(pre_act)
    return sigmoid_value * (1.0 + pre_act * (1.0 - sigmoid_value))


def reference(grid_latent, edge_latent, mesh_latent, mesh_grad, counts, request, edge_sender, edge_slot, w_send, w_recv, w_edge, edge_bias, w_out):
    scaled_grad = (mesh_grad.astype(jnp.float32) / counts.astype(jnp.float32)[:, None]).astype(jnp.bfloat16)
    node_proj = jnp.dot(mesh_latent, w_recv, preferred_element_type=jnp.float32)
    node_back = jnp.dot(scaled_grad, w_out.T, preferred_element_type=jnp.float32)
    recv_wide = w_recv.astype(jnp.float32)
    offsets = jnp.arange(SPAN, dtype=jnp.int32)

    def per_band(node_sum, band_index):
        grid_rows = lax.dynamic_slice_in_dim(grid_latent, band_index * G_DEV, G_DEV, 0)
        edge_rows = lax.dynamic_slice_in_dim(edge_latent, band_index * EDGE_DEV, EDGE_DEV, 0)
        senders = lax.dynamic_slice_in_dim(edge_sender, band_index * EDGE_DEV, EDGE_DEV, 0)
        slot_ids = lax.dynamic_slice_in_dim(edge_slot, band_index * EDGE_DEV, EDGE_DEV, 0)
        patches = (band_index + offsets - REACH).astype(jnp.int32)
        inside = (patches >= 0) & (patches < N_BAND)
        patch_clip = jnp.clip(patches, 0, N_BAND - 1).astype(jnp.int32)
        slot_table = request[patch_clip, offsets]
        slot_table = jnp.where(inside[:, None], slot_table, -1).reshape(-1)
        local_node = slot_table[slot_ids]
        patch_of = patch_clip[slot_ids // CAPACITY]
        is_live = (local_node >= 0)[:, None]
        receiver = (patch_of * M_DEV + jnp.maximum(local_node, 0)).astype(jnp.int32)
        grid_proj = jnp.dot(grid_rows, w_send, preferred_element_type=jnp.float32)
        pre_act = grid_proj[senders] + jnp.where(is_live, node_proj[receiver], 0.0)
        pre_act = pre_act + jnp.dot(edge_rows, w_edge, preferred_element_type=jnp.float32) + edge_bias.astype(jnp.float32)
        edge_grad = (jnp.where(is_live, node_back[receiver], 0.0) * silu_slope(pre_act)).astype(jnp.bfloat16)
        wide_grad = edge_grad.astype(jnp.float32)
        sender_sum = jax.ops.segment_sum(wide_grad, senders, num_segments=G_DEV).astype(jnp.bfloat16)
        grid_block = jnp.dot(sender_sum, w_send.T, preferred_element_type=jnp.float32).astype(jnp.bfloat16)
        node_sum = node_sum.at[receiver].add(jnp.where(is_live, wide_grad, 0.0))
        return node_sum, grid_block

    initial = jnp.zeros((M_DEV * N_BAND, HIDDEN_SIZE), jnp.float32)
    node_sum, grid_blocks = lax.scan(per_band, initial, jnp.arange(N_BAND, dtype=jnp.int32))
    grid_grad = grid_blocks.reshape(G_DEV * N_BAND, LATENT)
    node_grad = jnp.dot(node_sum, recv_wide.T, precision=lax.Precision.HIGHEST).astype(jnp.bfloat16)
    return grid_grad, node_grad
```

```python
import functools
import math

import jax
import jax.numpy as jnp
from jax import lax
from jax.experimental import pallas as pl
from jax.experimental.pallas import tpu as pltpu
from jax.sharding import PartitionSpec as P


def shifted(shard, axis, by):
    devices = lax.axis_size(axis)
    pairs = [(i, i + by) for i in range(devices) if 0 <= i + by < devices]
    return lax.ppermute(shard, axis, pairs)


def silu_slope(pre_act):
    sigmoid_value = jax.nn.sigmoid(pre_act)
    return sigmoid_value * (1.0 + pre_act * (1.0 - sigmoid_value))


def per_offset(blocks, reach, sign, mover):
    results = []
    for offset in range(blocks.shape[0]):
        amount = sign * (reach - offset)
        if amount == 0:
            results.append(blocks[offset])
        else:
            results.append(mover(blocks[offset], amount))
    return jnp.stack(results)


def largest_divisor(total, highest):
    width = highest
    while total % width:
        width //= 2
    return width


def edge_kernel(
    anchors,
    sender_ref,
    slot_ref,
    grid_ref,
    edge_ref,
    table_ref,
    w_send_ref,
    w_edge_ref,
    bias_ref,
    sender_out,
    slot_out,
    proj,
    sender_acc,
    slot_acc,
    *,
    grid_blocks,
    grid_rows,
    block_count,
):
    step = pl.program_id(0)
    width = edge_ref.shape[0]
    hidden = w_send_ref.shape[1]
    slot_count = table_ref.shape[0]

    @pl.when(step == 0)
    def _():
        proj[pl.ds(grid_rows, width), :] = jnp.zeros((width, hidden), jnp.float32)
        sender_acc[...] = jnp.zeros_like(sender_acc)
        slot_acc[...] = jnp.zeros_like(slot_acc)

    @pl.when(step < grid_blocks)
    def _():
        proj[pl.ds(pl.multiple_of(step * width, width), width), :] = jnp.dot(
            grid_ref[...], w_send_ref[...], preferred_element_type=jnp.float32
        )

    anchor = anchors[step]
    local = sender_ref[0].astype(jnp.float32) - anchor.astype(jnp.float32)
    slots = slot_ref[0].astype(jnp.float32)
    lanes = lax.broadcasted_iota(jnp.int32, (width, 128), 1).astype(jnp.float32)
    local_col = jnp.broadcast_to(local, (128, width)).T
    slots_col = jnp.broadcast_to(slots, (128, width)).T

    def rows_pick(column, count):
        parts = [
            jnp.where(column - 128.0 * j == lanes, 1.0, 0.0).astype(jnp.bfloat16)
            for j in range(count // 128)
        ]
        return jnp.concatenate(parts, axis=1)

    def cols_pick(row, count):
        rows = lax.broadcasted_iota(jnp.int32, (count, width), 0).astype(jnp.float32)
        return jnp.where(rows == row, 1.0, 0.0).astype(jnp.bfloat16)

    window = proj[pl.ds(anchor, width), :].astype(jnp.bfloat16)
    pre_act = jnp.dot(edge_ref[...], w_edge_ref[...], preferred_element_type=jnp.float32)
    pre_act += jnp.dot(rows_pick(local_col, width), window, preferred_element_type=jnp.float32)
    both = jnp.dot(
        rows_pick(slots_col, slot_count), table_ref[...], preferred_element_type=jnp.float32
    )
    pre_act += both[:, :hidden] + bias_ref[...]
    edge_grad = (both[:, hidden:] * silu_slope(pre_act)).astype(jnp.bfloat16)
    sender_acc[pl.ds(anchor, width), :] += jnp.dot(
        cols_pick(local, width), edge_grad, preferred_element_type=jnp.float32
    )
    slot_acc[...] += jnp.dot(
        cols_pick(slots, slot_count), edge_grad, preferred_element_type=jnp.float32
    )

    @pl.when(step == block_count - 1)
    def _():
        sender_out[...] = sender_acc[pl.ds(0, grid_rows), :].astype(sender_out.dtype)
        slot_out[...] = slot_acc[...].astype(slot_out.dtype)


def edge_pass(grid_latent, edge_latent, table, edge_sender, edge_slot, w_send, w_edge, bias, slot_type):
    grid_rows, latent = grid_latent.shape
    edge_count = edge_latent.shape[0]
    hidden = w_send.shape[1]
    slot_count = table.shape[0]
    width = largest_divisor(math.gcd(edge_count, grid_rows), 512)
    block_count = edge_count // width
    grid_blocks = grid_rows // width
    senders = edge_sender.reshape(block_count, 1, width)
    slots = edge_slot.reshape(block_count, 1, width)
    return pl.pallas_call(
        functools.partial(
            edge_kernel, grid_blocks=grid_blocks, grid_rows=grid_rows, block_count=block_count
        ),
        grid_spec=pltpu.PrefetchScalarGridSpec(
            num_scalar_prefetch=1,
            grid=(block_count,),
            in_specs=[
                pl.BlockSpec((1, 1, width), lambda i, a: (i, 0, 0)),
                pl.BlockSpec((1, 1, width), lambda i, a: (i, 0, 0)),
                pl.BlockSpec((width, latent), lambda i, a: (jnp.minimum(i, grid_blocks - 1), 0)),
                pl.BlockSpec((width, latent), lambda i, a: (i, 0)),
                pl.BlockSpec(table.shape, lambda i, a: (0, 0)),
                pl.BlockSpec(w_send.shape, lambda i, a: (0, 0)),
                pl.BlockSpec(w_edge.shape, lambda i, a: (0, 0)),
                pl.BlockSpec((1, hidden), lambda i, a: (0, 0)),
            ],
            out_specs=[
                pl.BlockSpec((grid_rows, hidden), lambda i, a: (0, 0)),
                pl.BlockSpec((slot_count, hidden), lambda i, a: (0, 0)),
            ],
            scratch_shapes=[
                pltpu.VMEM((grid_rows + width, hidden), jnp.float32),
                pltpu.VMEM((grid_rows + width, hidden), jnp.float32),
                pltpu.VMEM((slot_count, hidden), jnp.float32),
            ],
        ),
        out_shape=[
            jax.ShapeDtypeStruct((grid_rows, hidden), jnp.bfloat16),
            jax.ShapeDtypeStruct((slot_count, hidden), slot_type),
        ],
        compiler_params=pltpu.CompilerParams(dimension_semantics=("arbitrary",)),
        cost_estimate=pl.CostEstimate(
            flops=10_000_000_000, bytes_accessed=12_000_000, transcendentals=0
        ),
        name="edge_pass",
    )(senders[:, 0, 0], senders, slots, grid_latent, edge_latent, table, w_send, w_edge, bias.reshape(1, hidden))


def per_device(
    grid_latent,
    edge_latent,
    mesh_latent,
    mesh_grad,
    counts,
    request,
    edge_sender,
    edge_slot,
    w_send,
    w_recv,
    w_edge,
    edge_bias,
    w_out,
):
    span = request.shape[1]
    capacity = request.shape[2]
    reach = (span - 1) // 2
    node_count = mesh_latent.shape[0]
    latent = grid_latent.shape[1]
    slot_count = span * capacity
    scaled_grad = (mesh_grad.astype(jnp.float32) / counts.astype(jnp.float32)[:, None]).astype(
        jnp.bfloat16
    )
    wanted = request[0]
    live_slot = (wanted >= 0)[:, :, None]
    picker = jnp.maximum(wanted, 0)
    flat_live = live_slot.reshape(slot_count, 1)
    flat_picker = picker.reshape(-1)
    send_both = jnp.stack(
        [
            jnp.where(live_slot, mesh_latent[picker], 0),
            jnp.where(live_slot, scaled_grad[picker], 0),
        ],
        axis=1,
    )
    got_part = per_offset(send_both, reach, 1, lambda block, amount: shifted(block, "band", amount))
    got = lax.all_gather(got_part, "mp", axis=3, tiled=True)
    slot_proj = jnp.dot(
        got[:, 0].reshape(slot_count, latent), w_recv, preferred_element_type=jnp.float32
    )
    slot_back = jnp.dot(
        got[:, 1].reshape(slot_count, latent), w_out.T, preferred_element_type=jnp.float32
    )
    table = jnp.concatenate([slot_proj, slot_back], axis=1).astype(jnp.bfloat16)
    sender_sum, slot_sum = edge_pass(
        grid_latent, edge_latent, table, edge_sender, edge_slot, w_send, w_edge, edge_bias, jnp.float32
    )
    recv_wide = w_recv.astype(jnp.float32)
    slot_term = jnp.dot(slot_sum, recv_wide.T, precision=lax.Precision.HIGHEST)
    slot_share = lax.psum_scatter(
        slot_term.astype(jnp.bfloat16), "mp", scatter_dimension=1, tiled=True
    ).astype(jnp.float32)
    part_cols = slot_share.shape[1]
    returned = per_offset(
        slot_share.reshape(span, capacity, part_cols),
        reach,
        -1,
        lambda block, amount: shifted(block.astype(jnp.bfloat16), "band", amount).astype(
            block.dtype
        ),
    )
    kept_rows = jnp.where(flat_live, returned.reshape(slot_count, part_cols), 0.0)
    node_grad = jax.ops.segment_sum(kept_rows, flat_picker, num_segments=node_count).astype(
        jnp.bfloat16
    )
    grid_term = jnp.dot(sender_sum, w_send.T, preferred_element_type=jnp.float32)
    grid_grad = lax.psum_scatter(
        grid_term.astype(jnp.bfloat16), "mp", scatter_dimension=1, tiled=True
    )
    return (grid_grad, node_grad)


def solution(mesh):
    in_specs = (
        P("band", None),
        P("band", None),
        P("band", "mp"),
        P("band", "mp"),
        P("band"),
        P("band", None, None),
        P("band"),
        P("band"),
        P(None, "mp"),
        P(None, "mp"),
        P(None, "mp"),
        P("mp"),
        P("mp", None),
    )
    out_specs = (P("band", "mp"), P("band", "mp"))
    return jax.shard_map(
        per_device, mesh=mesh, in_specs=in_specs, out_specs=out_specs, check_vma=False
    )
```

```python
import functools
import math

import jax
import jax.numpy as jnp
from jax import lax
from jax.experimental import pallas as pl
from jax.experimental.pallas import tpu as pltpu
from jax.sharding import PartitionSpec as P


def silu_slope(pre_act):
    sigmoid_value = jax.nn.sigmoid(pre_act)
    return sigmoid_value * (1.0 + pre_act * (1.0 - sigmoid_value))


def largest_divisor(total, highest):
    width = highest
    while total % width:
        width //= 2
    return width


def edge_kernel(
    anchors,
    sender_ref,
    slot_ref,
    grid_ref,
    edge_ref,
    table_ref,
    w_send_ref,
    w_edge_ref,
    bias_ref,
    sender_out,
    slot_out,
    proj,
    sender_acc,
    slot_acc,
    *,
    grid_blocks,
    grid_rows,
    block_count,
):
    step = pl.program_id(0)
    width = edge_ref.shape[0]
    hidden = w_send_ref.shape[1]
    slot_count = table_ref.shape[0]

    @pl.when(step == 0)
    def _():
        proj[pl.ds(grid_rows, width), :] = jnp.zeros((width, hidden), jnp.float32)
        sender_acc[...] = jnp.zeros_like(sender_acc)
        slot_acc[...] = jnp.zeros_like(slot_acc)

    @pl.when(step < grid_blocks)
    def _():
        proj[pl.ds(pl.multiple_of(step * width, width), width), :] = jnp.dot(
            grid_ref[...], w_send_ref[...], preferred_element_type=jnp.float32
        )

    anchor = anchors[step]
    local = sender_ref[0].astype(jnp.float32) - anchor.astype(jnp.float32)
    slots = slot_ref[0].astype(jnp.float32)
    lanes = lax.broadcasted_iota(jnp.int32, (width, 128), 1).astype(jnp.float32)
    local_col = jnp.broadcast_to(local, (128, width)).T
    slots_col = jnp.broadcast_to(slots, (128, width)).T

    def rows_pick(column, count):
        parts = [
            jnp.where(column - 128.0 * j == lanes, 1.0, 0.0).astype(jnp.bfloat16)
            for j in range(count // 128)
        ]
        return jnp.concatenate(parts, axis=1)

    def cols_pick(row, count):
        rows = lax.broadcasted_iota(jnp.int32, (count, width), 0).astype(jnp.float32)
        return jnp.where(rows == row, 1.0, 0.0).astype(jnp.bfloat16)

    window = proj[pl.ds(anchor, width), :].astype(jnp.bfloat16)
    pre_act = jnp.dot(edge_ref[...], w_edge_ref[...], preferred_element_type=jnp.float32)
    pre_act += jnp.dot(rows_pick(local_col, width), window, preferred_element_type=jnp.float32)
    both = jnp.dot(
        rows_pick(slots_col, slot_count), table_ref[...], preferred_element_type=jnp.float32
    )
    pre_act += both[:, :hidden] + bias_ref[...]
    edge_grad = (both[:, hidden:] * silu_slope(pre_act)).astype(jnp.bfloat16)
    sender_acc[pl.ds(anchor, width), :] += jnp.dot(
        cols_pick(local, width), edge_grad, preferred_element_type=jnp.float32
    )
    slot_acc[...] += jnp.dot(
        cols_pick(slots, slot_count), edge_grad, preferred_element_type=jnp.float32
    )

    @pl.when(step == block_count - 1)
    def _():
        sender_out[...] = sender_acc[pl.ds(0, grid_rows), :].astype(sender_out.dtype)
        slot_out[...] = slot_acc[...].astype(slot_out.dtype)


def edge_pass(grid_latent, edge_latent, table, edge_sender, edge_slot, w_send, w_edge, bias, slot_type):
    grid_rows, latent = grid_latent.shape
    edge_count = edge_latent.shape[0]
    hidden = w_send.shape[1]
    slot_count = table.shape[0]
    width = largest_divisor(math.gcd(edge_count, grid_rows), 512)
    block_count = edge_count // width
    grid_blocks = grid_rows // width
    senders = edge_sender.reshape(block_count, 1, width)
    slots = edge_slot.reshape(block_count, 1, width)
    return pl.pallas_call(
        functools.partial(
            edge_kernel, grid_blocks=grid_blocks, grid_rows=grid_rows, block_count=block_count
        ),
        grid_spec=pltpu.PrefetchScalarGridSpec(
            num_scalar_prefetch=1,
            grid=(block_count,),
            in_specs=[
                pl.BlockSpec((1, 1, width), lambda i, a: (i, 0, 0)),
                pl.BlockSpec((1, 1, width), lambda i, a: (i, 0, 0)),
                pl.BlockSpec((width, latent), lambda i, a: (jnp.minimum(i, grid_blocks - 1), 0)),
                pl.BlockSpec((width, latent), lambda i, a: (i, 0)),
                pl.BlockSpec(table.shape, lambda i, a: (0, 0)),
                pl.BlockSpec(w_send.shape, lambda i, a: (0, 0)),
                pl.BlockSpec(w_edge.shape, lambda i, a: (0, 0)),
                pl.BlockSpec((1, hidden), lambda i, a: (0, 0)),
            ],
            out_specs=[
                pl.BlockSpec((grid_rows, hidden), lambda i, a: (0, 0)),
                pl.BlockSpec((slot_count, hidden), lambda i, a: (0, 0)),
            ],
            scratch_shapes=[
                pltpu.VMEM((grid_rows + width, hidden), jnp.float32),
                pltpu.VMEM((grid_rows + width, hidden), jnp.float32),
                pltpu.VMEM((slot_count, hidden), jnp.float32),
            ],
        ),
        out_shape=[
            jax.ShapeDtypeStruct((grid_rows, hidden), jnp.bfloat16),
            jax.ShapeDtypeStruct((slot_count, hidden), slot_type),
        ],
        compiler_params=pltpu.CompilerParams(dimension_semantics=("arbitrary",)),
        cost_estimate=pl.CostEstimate(
            flops=10_000_000_000, bytes_accessed=12_000_000, transcendentals=0
        ),
        name="edge_pass",
    )(senders[:, 0, 0], senders, slots, grid_latent, edge_latent, table, w_send, w_edge, bias.reshape(1, hidden))


MESH_ID = pl.DeviceIdType.MESH
DIMS_NT = (((1,), (1,)), ((), ()))


def greet(reach):
    band = lax.axis_index("band")
    bands = lax.axis_size("band")
    part = lax.axis_index("mp")
    parts = lax.axis_size("mp")
    barrier = pltpu.get_barrier_semaphore()
    for turn in range(1, parts):
        pl.semaphore_signal(
            barrier, inc=1, device_id=(band, lax.rem(part + turn, parts)), device_id_type=MESH_ID
        )
    shifts = [by for by in range(-reach, reach + 1) if by != 0]
    for by in shifts:
        @pl.when((band + by >= 0) & (band + by < bands))
        def _():
            pl.semaphore_signal(barrier, inc=1, device_id=(band + by, part), device_id_type=MESH_ID)

    below = jnp.minimum(band, reach)
    above = jnp.minimum(bands - 1 - band, reach)
    pl.semaphore_wait(barrier, parts - 1 + below + above)


def spread_kernel(
    rows_ref, wanted_ref, w_recv_ref, w_out_ref, rows_w_ref,
    table_ref, weight_ref,
    held, both, stage, landed, weight_land,
    near_send, near_recv, far_send, far_recv, pass_send, pass_recv,
    band_send, band_recv, weight_send, weight_recv,
    *, reach,
):
    band = lax.axis_index("band")
    bands = lax.axis_size("band")
    part = lax.axis_index("mp")
    parts = lax.axis_size("mp")
    across = lax.rem(part + parts // 2, parts)
    beside = part + 1 - 2 * lax.rem(part, 2)
    span, capacity = wanted_ref.shape
    node_count, twice = rows_ref.shape
    cols = twice // 2
    hidden = w_recv_ref.shape[1]
    greet(reach)

    def remote(source, target, send, recv, device):
        return pltpu.make_async_remote_copy(
            src_ref=source, dst_ref=target, send_sem=send, recv_sem=recv,
            device_id=device, device_id_type=MESH_ID,
        )

    far = remote(rows_ref, held.at[part], far_send, far_recv, (band, across))
    near = remote(rows_ref, held.at[part], near_send, near_recv, (band, beside))
    far.start()
    near.start()
    weight_rows = rows_w_ref.shape[0] // parts
    moves = []
    for turn in range(1, parts):
        peer = lax.rem(part + turn, parts)
        move = remote(
            rows_w_ref.at[pl.ds(pl.multiple_of(peer * weight_rows, weight_rows), weight_rows), :],
            weight_land.at[part], weight_send.at[turn], weight_recv.at[turn], (band, peer),
        )
        move.start()
        moves.append(move)
    weight_land[part] = rows_w_ref[
        pl.ds(pl.multiple_of(part * weight_rows, weight_rows), weight_rows), :
    ]
    held[part] = rows_ref[...]
    far.wait_recv()
    onward = remote(held.at[across], held.at[across], pass_send, pass_recv, (band, beside))
    onward.start()
    near.wait_recv()
    onward.wait_recv()
    ahead = jnp.zeros((node_count, hidden), jnp.float32)
    back = jnp.zeros((node_count, hidden), jnp.float32)
    for j in range(held.shape[0]):
        block = held[j]
        ahead += jnp.dot(
            block[:, :cols], w_recv_ref[j * cols : (j + 1) * cols, :],
            preferred_element_type=jnp.float32,
        )
        back += lax.dot_general(
            block[:, cols:], w_out_ref[:, j * cols : (j + 1) * cols], DIMS_NT,
            preferred_element_type=jnp.float32,
        )
    both[:, :hidden] = ahead.astype(both.dtype)
    both[:, hidden:] = back.astype(both.dtype)
    lanes = lax.broadcasted_iota(jnp.int32, (capacity, 128), 1).astype(jnp.float32)
    order = sorted(range(span), key=lambda k: -abs(k - reach))
    sends = {}
    for k in order:
        row = wanted_ref[k : k + 1, :].astype(jnp.float32)
        column = jnp.broadcast_to(row, (128, capacity)).T
        pick = jnp.concatenate(
            [
                jnp.where(column - 128.0 * j == lanes, 1.0, 0.0).astype(jnp.bfloat16)
                for j in range(node_count // 128)
            ],
            axis=1,
        )
        chosen = jnp.dot(pick, both[...], preferred_element_type=jnp.float32).astype(jnp.bfloat16)
        if k == reach:
            landed[k] = chosen
            continue
        stage[k] = chosen
        target = band + reach - k
        sends[k] = remote(
            stage.at[k], landed.at[k], band_send.at[k], band_recv.at[k], (target, part)
        )

        @pl.when((target >= 0) & (target < bands))
        def _():
            sends[k].start()

        source = band + k - reach

        @pl.when((source < 0) | (source >= bands))
        def _():
            landed[k] = jnp.zeros((capacity, 2 * hidden), landed.dtype)

    for move in moves:
        move.wait_recv()
    weight_ref[...] = weight_land[...]
    for k in reversed(order):
        if k == reach:
            continue
        source = band + k - reach

        @pl.when((source >= 0) & (source < bands))
        def _():
            sends[k].wait_recv()

    table_ref[...] = landed[...].reshape(span * capacity, 2 * hidden)
    far.wait_send()
    near.wait_send()
    onward.wait_send()
    for move in moves:
        move.wait_send()
    for k in order:
        if k == reach:
            continue
        target = band + reach - k

        @pl.when((target >= 0) & (target < bands))
        def _():
            sends[k].wait_send()


VMEM_SPEC = pl.BlockSpec(memory_space=pltpu.VMEM)
DMA_SEM = pltpu.SemaphoreType.DMA


def spread(rows, wanted, w_recv, w_out, rows_w, parts, reach):
    span, capacity = wanted.shape
    node_count, twice = rows.shape
    hidden = w_recv.shape[1]
    weight_shape = (parts, rows_w.shape[0] // parts, rows_w.shape[1])
    return pl.pallas_call(
        functools.partial(spread_kernel, reach=reach),
        in_specs=[VMEM_SPEC] * 5,
        out_specs=[VMEM_SPEC] * 2,
        out_shape=[
            jax.ShapeDtypeStruct((span * capacity, 2 * hidden), jnp.bfloat16),
            jax.ShapeDtypeStruct(weight_shape, jnp.bfloat16),
        ],
        scratch_shapes=[
            pltpu.VMEM((parts, node_count, twice), jnp.bfloat16),
            pltpu.VMEM((node_count, 2 * hidden), jnp.bfloat16),
            pltpu.VMEM((span, capacity, 2 * hidden), jnp.bfloat16),
            pltpu.VMEM((span, capacity, 2 * hidden), jnp.bfloat16),
            pltpu.VMEM(weight_shape, jnp.bfloat16),
        ]
        + [DMA_SEM] * 6
        + [DMA_SEM((span,)), DMA_SEM((span,)), DMA_SEM((parts,)), DMA_SEM((parts,))],
        compiler_params=pltpu.CompilerParams(collective_id=0, has_side_effects=True),
        name="spread",
    )(rows, wanted, w_recv, w_out, rows_w)


def collect_kernel(
    slot_ref, sender_ref, wanted_ref, weight_ref,
    grid_ref, node_ref,
    back, held, node_stage, node_held,
    band_send, band_recv, near_send, near_recv, far_send, far_recv, pass_send, pass_recv,
    *, reach, chunks,
):
    band = lax.axis_index("band")
    bands = lax.axis_size("band")
    part = lax.axis_index("mp")
    parts = lax.axis_size("mp")
    across = lax.rem(part + parts // 2, parts)
    beside = part + 1 - 2 * lax.rem(part, 2)
    span, capacity = wanted_ref.shape
    node_count, hidden = node_stage.shape
    rows = sender_ref.shape[0] // chunks
    greet(reach)

    def remote(source, target, send, recv, device):
        return pltpu.make_async_remote_copy(
            src_ref=source, dst_ref=target, send_sem=send, recv_sem=recv,
            device_id=device, device_id_type=MESH_ID,
        )

    order = [k for k in sorted(range(span), key=lambda k: -abs(k - reach)) if k != reach]
    sends = {}
    for k in order:
        target = band + k - reach
        sends[k] = remote(
            slot_ref.at[k], back.at[k], band_send.at[k], band_recv.at[k], (target, part)
        )

        @pl.when((target >= 0) & (target < bands))
        def _():
            sends[k].start()

    def slab(index):
        return pl.ds(index * rows, rows)

    fars, nears, onwards = [], [], []
    for c in range(chunks):
        source = sender_ref.at[slab(c), :]
        fars.append(
            remote(source, held.at[part, slab(c), :], far_send.at[c], far_recv.at[c], (band, across))
        )
        nears.append(
            remote(source, held.at[part, slab(c), :], near_send.at[c], near_recv.at[c], (band, beside))
        )
        fars[c].start()
        nears[c].start()
    held[part] = sender_ref[...]

    def node_row(k):
        ids = lax.broadcasted_iota(jnp.int32, (node_count, capacity), 0)
        return jnp.where(ids == wanted_ref[k : k + 1, :], 1.0, 0.0).astype(jnp.bfloat16)

    node_sum = jnp.dot(node_row(reach), slot_ref[reach], preferred_element_type=jnp.float32)
    for k in reversed(order):
        source = band + reach - k

        @pl.when((source >= 0) & (source < bands))
        def _():
            sends[k].wait_recv()

        @pl.when((source < 0) | (source >= bands))
        def _():
            back[k] = jnp.zeros((capacity, hidden), back.dtype)

        node_sum += jnp.dot(node_row(k), back[k], preferred_element_type=jnp.float32)
    node_stage[...] = node_sum.astype(node_stage.dtype)
    node_held[part] = node_sum.astype(node_held.dtype)
    fars.append(
        remote(node_stage, node_held.at[part], far_send.at[chunks], far_recv.at[chunks], (band, across))
    )
    nears.append(
        remote(node_stage, node_held.at[part], near_send.at[chunks], near_recv.at[chunks], (band, beside))
    )
    fars[chunks].start()
    nears[chunks].start()

    def pass_on(c):
        fars[c].wait_recv()
        block = held.at[across, slab(c), :] if c < chunks else node_held.at[across]
        onwards.append(remote(block, block, pass_send.at[c], pass_recv.at[c], (band, beside)))
        onwards[c].start()

    def finish(c):
        nears[c].wait_recv()
        onwards[c].wait_recv()
        if c < chunks:
            blocks = [held[j, c * rows : (c + 1) * rows, :] for j in range(held.shape[0])]
            weights = [weight_ref[j, :, :hidden] for j in range(held.shape[0])]
        else:
            blocks = [node_held[j] for j in range(held.shape[0])]
            weights = [weight_ref[j, :, hidden:] for j in range(held.shape[0])]
        total = lax.dot_general(
            jnp.concatenate(blocks, axis=1), jnp.concatenate(weights, axis=1), DIMS_NT,
            preferred_element_type=jnp.float32,
        )
        if c < chunks:
            grid_ref[c * rows : (c + 1) * rows, :] = total.astype(grid_ref.dtype)
        else:
            node_ref[...] = total.astype(node_ref.dtype)

    for c in range(chunks + 1):
        pass_on(c)
        if c > 0:
            finish(c - 1)
    finish(chunks)
    for c in range(chunks + 1):
        fars[c].wait_send()
        nears[c].wait_send()
        onwards[c].wait_send()
    for k in order:
        target = band + k - reach

        @pl.when((target >= 0) & (target < bands))
        def _():
            sends[k].wait_send()


def collect(slot_sum, sender_sum, wanted, weights, node_count, reach):
    span, capacity = wanted.shape
    grid_rows, hidden = sender_sum.shape
    parts, out_cols, _ = weights.shape
    chunks = 4
    tokens = chunks + 1
    return pl.pallas_call(
        functools.partial(collect_kernel, reach=reach, chunks=chunks),
        in_specs=[VMEM_SPEC] * 4,
        out_specs=[VMEM_SPEC] * 2,
        out_shape=[
            jax.ShapeDtypeStruct((grid_rows, out_cols), jnp.bfloat16),
            jax.ShapeDtypeStruct((node_count, out_cols), jnp.bfloat16),
        ],
        scratch_shapes=[
            pltpu.VMEM((span, capacity, hidden), jnp.bfloat16),
            pltpu.VMEM((parts, grid_rows, hidden), jnp.bfloat16),
            pltpu.VMEM((node_count, hidden), jnp.bfloat16),
            pltpu.VMEM((parts, node_count, hidden), jnp.bfloat16),
        ]
        + [DMA_SEM((span,))] * 2
        + [DMA_SEM((tokens,))] * 6,
        compiler_params=pltpu.CompilerParams(collective_id=1, has_side_effects=True),
        name="collect",
    )(slot_sum.reshape(span, capacity, hidden), sender_sum, wanted, weights)


def per_device(
    grid_latent,
    edge_latent,
    mesh_latent,
    mesh_grad,
    counts,
    request,
    edge_sender,
    edge_slot,
    w_send,
    w_recv,
    w_edge,
    edge_bias,
    w_out,
):
    span = request.shape[1]
    reach = (span - 1) // 2
    parts = lax.axis_size("mp")
    scaled_grad = (mesh_grad.astype(jnp.float32) / counts.astype(jnp.float32)[:, None]).astype(
        jnp.bfloat16
    )
    wanted = request[0]
    table, weights = spread(
        jnp.concatenate([mesh_latent, scaled_grad], axis=1),
        wanted,
        w_recv,
        w_out,
        jnp.concatenate([w_send, w_recv], axis=1),
        parts,
        reach,
    )
    sender_sum, slot_sum = edge_pass(
        grid_latent, edge_latent, table, edge_sender, edge_slot, w_send, w_edge, edge_bias, jnp.bfloat16
    )
    return tuple(collect(slot_sum, sender_sum, wanted, weights, mesh_latent.shape[0], reach))


def solution(mesh):
    in_specs = (
        P("band", None),
        P("band", None),
        P("band", "mp"),
        P("band", "mp"),
        P("band"),
        P("band", None, None),
        P("band"),
        P("band"),
        P(None, "mp"),
        P(None, "mp"),
        P(None, "mp"),
        P("mp"),
        P("mp", None),
    )
    out_specs = (P("band", "mp"), P("band", "mp"))
    return jax.shard_map(
        per_device, mesh=mesh, in_specs=in_specs, out_specs=out_specs, check_vma=False
    )
```

```python
import functools
import math

import jax
import jax.numpy as jnp
from jax import lax
from jax.experimental import pallas as pl
from jax.experimental.pallas import tpu as pltpu
from jax.sharding import PartitionSpec as P


def silu_slope(pre_act):
    sigmoid_value = jax.nn.sigmoid(pre_act)
    return sigmoid_value * (1.0 + pre_act * (1.0 - sigmoid_value))


def largest_divisor(total, highest):
    width = highest
    while total % width:
        width //= 2
    return width


def edge_kernel(
    anchors,
    sender_ref,
    slot_ref,
    grid_ref,
    edge_ref,
    table_ref,
    w_send_ref,
    w_edge_ref,
    bias_ref,
    sender_out,
    slot_out,
    proj,
    sender_acc,
    slot_acc,
    *,
    grid_blocks,
    grid_rows,
    block_count,
):
    step = pl.program_id(0)
    width = edge_ref.shape[0]
    hidden = w_send_ref.shape[1]
    slot_count = table_ref.shape[0]

    @pl.when(step == 0)
    def _():
        proj[pl.ds(grid_rows, width), :] = jnp.zeros((width, hidden), jnp.float32)
        sender_acc[...] = jnp.zeros_like(sender_acc)
        slot_acc[...] = jnp.zeros_like(slot_acc)

    @pl.when(step < grid_blocks)
    def _():
        proj[pl.ds(pl.multiple_of(step * width, width), width), :] = jnp.dot(
            grid_ref[...], w_send_ref[...], preferred_element_type=jnp.float32
        )

    anchor = anchors[step * width]
    local = sender_ref[0].astype(jnp.float32) - anchor.astype(jnp.float32)
    slots = slot_ref[0].astype(jnp.float32)
    lanes = lax.broadcasted_iota(jnp.int32, (width, 128), 1).astype(jnp.float32)
    local_col = jnp.broadcast_to(local, (128, width)).T
    slots_col = jnp.broadcast_to(slots, (128, width)).T

    def rows_pick(column, count):
        parts = [
            jnp.where(column - 128.0 * j == lanes, 1.0, 0.0).astype(jnp.bfloat16)
            for j in range(count // 128)
        ]
        return jnp.concatenate(parts, axis=1)

    def cols_pick(row, count):
        rows = lax.broadcasted_iota(jnp.int32, (count, width), 0).astype(jnp.float32)
        return jnp.where(rows == row, 1.0, 0.0).astype(jnp.bfloat16)

    window = proj[pl.ds(anchor, width), :].astype(jnp.bfloat16)
    pre_act = jnp.dot(edge_ref[...], w_edge_ref[...], preferred_element_type=jnp.float32)
    pre_act += jnp.dot(rows_pick(local_col, width), window, preferred_element_type=jnp.float32)
    both = jnp.dot(
        rows_pick(slots_col, slot_count), table_ref[...], preferred_element_type=jnp.float32
    )
    pre_act += both[:, :hidden] + bias_ref[...]
    edge_grad = (both[:, hidden:] * silu_slope(pre_act)).astype(jnp.bfloat16)
    sender_acc[pl.ds(anchor, width), :] += jnp.dot(
        cols_pick(local, width), edge_grad, preferred_element_type=jnp.float32
    )
    slot_acc[...] += jnp.dot(
        cols_pick(slots, slot_count), edge_grad, preferred_element_type=jnp.float32
    )

    @pl.when(step == block_count - 1)
    def _():
        sender_out[...] = sender_acc[pl.ds(0, grid_rows), :].astype(sender_out.dtype)
        slot_out[...] = slot_acc[...].astype(slot_out.dtype)


def edge_pass(grid_latent, edge_latent, table, edge_sender, edge_slot, w_send, w_edge, bias, slot_type):
    grid_rows, latent = grid_latent.shape
    edge_count = edge_latent.shape[0]
    hidden = w_send.shape[1]
    slot_count = table.shape[0]
    width = largest_divisor(math.gcd(edge_count, grid_rows), 512)
    block_count = edge_count // width
    grid_blocks = grid_rows // width
    senders = edge_sender.reshape(block_count, 1, width)
    slots = edge_slot.reshape(block_count, 1, width)
    return pl.pallas_call(
        functools.partial(
            edge_kernel, grid_blocks=grid_blocks, grid_rows=grid_rows, block_count=block_count
        ),
        grid_spec=pltpu.PrefetchScalarGridSpec(
            num_scalar_prefetch=1,
            grid=(block_count,),
            in_specs=[
                pl.BlockSpec((1, 1, width), lambda i, a: (i, 0, 0)),
                pl.BlockSpec((1, 1, width), lambda i, a: (i, 0, 0)),
                pl.BlockSpec((width, latent), lambda i, a: (jnp.minimum(i, grid_blocks - 1), 0)),
                pl.BlockSpec((width, latent), lambda i, a: (i, 0)),
                pl.BlockSpec(table.shape, lambda i, a: (0, 0)),
                pl.BlockSpec(w_send.shape, lambda i, a: (0, 0)),
                pl.BlockSpec(w_edge.shape, lambda i, a: (0, 0)),
                pl.BlockSpec((1, hidden), lambda i, a: (0, 0)),
            ],
            out_specs=[
                pl.BlockSpec((grid_rows, hidden), lambda i, a: (0, 0)),
                pl.BlockSpec((slot_count, hidden), lambda i, a: (0, 0)),
            ],
            scratch_shapes=[
                pltpu.VMEM((grid_rows + width, hidden), jnp.float32),
                pltpu.VMEM((grid_rows + width, hidden), jnp.float32),
                pltpu.VMEM((slot_count, hidden), jnp.float32),
            ],
        ),
        out_shape=[
            jax.ShapeDtypeStruct((grid_rows, hidden), jnp.bfloat16),
            jax.ShapeDtypeStruct((slot_count, hidden), slot_type),
        ],
        compiler_params=pltpu.CompilerParams(dimension_semantics=("arbitrary",)),
        cost_estimate=pl.CostEstimate(
            flops=10_000_000_000, bytes_accessed=12_000_000, transcendentals=0
        ),
        name="edge_pass",
    )(edge_sender, senders, slots, grid_latent, edge_latent, table, w_send, w_edge, bias.reshape(1, hidden))


MESH_ID = pl.DeviceIdType.MESH
DIMS_NT = (((1,), (1,)), ((), ()))


def greet(reach):
    band = lax.axis_index("band")
    bands = lax.axis_size("band")
    part = lax.axis_index("mp")
    parts = lax.axis_size("mp")
    barrier = pltpu.get_barrier_semaphore()
    for turn in range(1, parts):
        pl.semaphore_signal(
            barrier, inc=1, device_id=(band, lax.rem(part + turn, parts)), device_id_type=MESH_ID
        )
    shifts = [by for by in range(-reach, reach + 1) if by != 0]
    for by in shifts:
        @pl.when((band + by >= 0) & (band + by < bands))
        def _():
            pl.semaphore_signal(barrier, inc=1, device_id=(band + by, part), device_id_type=MESH_ID)

    below = jnp.minimum(band, reach)
    above = jnp.minimum(bands - 1 - band, reach)
    pl.semaphore_wait(barrier, parts - 1 + below + above)


def spread_kernel(
    latent_ref, grad_ref, counts_ref, wanted_ref, w_recv_ref, w_out_ref, w_send_ref,
    table_ref, weight_ref,
    held, both, stage, landed, weight_land,
    near_send, near_recv, far_send, far_recv, pass_send, pass_recv,
    band_send, band_recv, weight_send, weight_recv,
    *, reach,
):
    band = lax.axis_index("band")
    bands = lax.axis_size("band")
    part = lax.axis_index("mp")
    parts = lax.axis_size("mp")
    across = lax.rem(part + parts // 2, parts)
    beside = part + 1 - 2 * lax.rem(part, 2)
    span, capacity = wanted_ref.shape
    node_count, cols = latent_ref.shape
    hidden = w_recv_ref.shape[1]
    count_row = counts_ref[...].astype(jnp.float32)
    count_col = jnp.broadcast_to(count_row, (cols, node_count)).T
    held[part, :, :cols] = latent_ref[...]
    held[part, :, cols:] = (grad_ref[...].astype(jnp.float32) / count_col).astype(held.dtype)
    weight_rows = w_send_ref.shape[0] // parts
    own_rows = pl.ds(pl.multiple_of(part * weight_rows, weight_rows), weight_rows)
    weight_land[0, part] = w_send_ref[own_rows, :]
    weight_land[1, part] = w_recv_ref[own_rows, :]
    greet(reach)

    def remote(source, target, send, recv, device):
        return pltpu.make_async_remote_copy(
            src_ref=source, dst_ref=target, send_sem=send, recv_sem=recv,
            device_id=device, device_id_type=MESH_ID,
        )

    far = remote(held.at[part], held.at[part], far_send, far_recv, (band, across))
    near = remote(held.at[part], held.at[part], near_send, near_recv, (band, beside))
    far.start()
    near.start()
    moves = []
    for turn in range(1, parts):
        peer = lax.rem(part + turn, parts)
        peer_rows = pl.ds(pl.multiple_of(peer * weight_rows, weight_rows), weight_rows)
        for which, ref in enumerate((w_send_ref, w_recv_ref)):
            move = remote(
                ref.at[peer_rows, :], weight_land.at[which, part],
                weight_send.at[which, turn], weight_recv.at[which, turn], (band, peer),
            )
            move.start()
            moves.append(move)
    far.wait_recv()
    onward = remote(held.at[across], held.at[across], pass_send, pass_recv, (band, beside))
    onward.start()
    near.wait_recv()
    onward.wait_recv()
    ahead = jnp.zeros((node_count, hidden), jnp.float32)
    back = jnp.zeros((node_count, hidden), jnp.float32)
    for j in range(held.shape[0]):
        block = held[j]
        ahead += jnp.dot(
            block[:, :cols], w_recv_ref[j * cols : (j + 1) * cols, :],
            preferred_element_type=jnp.float32,
        )
        back += lax.dot_general(
            block[:, cols:], w_out_ref[:, j * cols : (j + 1) * cols], DIMS_NT,
            preferred_element_type=jnp.float32,
        )
    both[:, :hidden] = ahead.astype(both.dtype)
    both[:, hidden:] = back.astype(both.dtype)
    lanes = lax.broadcasted_iota(jnp.int32, (capacity, 128), 1).astype(jnp.float32)
    order = sorted(range(span), key=lambda k: -abs(k - reach))
    sends = {}
    for k in order:
        row = wanted_ref[k : k + 1, :].astype(jnp.float32)
        column = jnp.broadcast_to(row, (128, capacity)).T
        pick = jnp.concatenate(
            [
                jnp.where(column - 128.0 * j == lanes, 1.0, 0.0).astype(jnp.bfloat16)
                for j in range(node_count // 128)
            ],
            axis=1,
        )
        chosen = jnp.dot(pick, both[...], preferred_element_type=jnp.float32).astype(jnp.bfloat16)
        if k == reach:
            landed[k] = chosen
            continue
        stage[k] = chosen
        target = band + reach - k
        sends[k] = remote(
            stage.at[k], landed.at[k], band_send.at[k], band_recv.at[k], (target, part)
        )

        @pl.when((target >= 0) & (target < bands))
        def _():
            sends[k].start()

        source = band + k - reach

        @pl.when((source < 0) | (source >= bands))
        def _():
            landed[k] = jnp.zeros((capacity, 2 * hidden), landed.dtype)

    for move in moves:
        move.wait_recv()
    weight_ref[...] = weight_land[...]
    for k in reversed(order):
        if k == reach:
            continue
        source = band + k - reach

        @pl.when((source >= 0) & (source < bands))
        def _():
            sends[k].wait_recv()

    table_ref[...] = landed[...].reshape(span * capacity, 2 * hidden)
    far.wait_send()
    near.wait_send()
    onward.wait_send()
    for move in moves:
        move.wait_send()
    for k in order:
        if k == reach:
            continue
        target = band + reach - k

        @pl.when((target >= 0) & (target < bands))
        def _():
            sends[k].wait_send()


VMEM_SPEC = pl.BlockSpec(memory_space=pltpu.VMEM)
DMA_SEM = pltpu.SemaphoreType.DMA


def spread(mesh_latent, mesh_grad, counts, wanted, w_recv, w_out, w_send, parts, reach):
    span, capacity = wanted.shape
    node_count, cols = mesh_latent.shape
    hidden = w_recv.shape[1]
    weight_shape = (2, parts, w_send.shape[0] // parts, hidden)
    return pl.pallas_call(
        functools.partial(spread_kernel, reach=reach),
        in_specs=[VMEM_SPEC] * 7,
        out_specs=[VMEM_SPEC] * 2,
        out_shape=[
            jax.ShapeDtypeStruct((span * capacity, 2 * hidden), jnp.bfloat16),
            jax.ShapeDtypeStruct(weight_shape, jnp.bfloat16),
        ],
        scratch_shapes=[
            pltpu.VMEM((parts, node_count, 2 * cols), jnp.bfloat16),
            pltpu.VMEM((node_count, 2 * hidden), jnp.bfloat16),
            pltpu.VMEM((span, capacity, 2 * hidden), jnp.bfloat16),
            pltpu.VMEM((span, capacity, 2 * hidden), jnp.bfloat16),
            pltpu.VMEM(weight_shape, jnp.bfloat16),
        ]
        + [DMA_SEM] * 6
        + [DMA_SEM((span,)), DMA_SEM((span,)), DMA_SEM((2, parts)), DMA_SEM((2, parts))],
        compiler_params=pltpu.CompilerParams(collective_id=0, has_side_effects=True),
        name="spread",
    )(mesh_latent, mesh_grad, counts.reshape(1, node_count), wanted, w_recv, w_out, w_send)


def collect_kernel(
    slot_ref, sender_ref, wanted_ref, weight_ref,
    grid_ref, node_ref,
    back, held, node_stage, node_held,
    band_send, band_recv, near_send, near_recv, far_send, far_recv, pass_send, pass_recv,
    *, reach, chunks,
):
    band = lax.axis_index("band")
    bands = lax.axis_size("band")
    part = lax.axis_index("mp")
    parts = lax.axis_size("mp")
    across = lax.rem(part + parts // 2, parts)
    beside = part + 1 - 2 * lax.rem(part, 2)
    span, capacity = wanted_ref.shape
    node_count, hidden = node_stage.shape
    rows = sender_ref.shape[0] // chunks
    greet(reach)

    def remote(source, target, send, recv, device):
        return pltpu.make_async_remote_copy(
            src_ref=source, dst_ref=target, send_sem=send, recv_sem=recv,
            device_id=device, device_id_type=MESH_ID,
        )

    order = [k for k in sorted(range(span), key=lambda k: -abs(k - reach)) if k != reach]
    sends = {}
    for k in order:
        target = band + k - reach
        sends[k] = remote(
            slot_ref.at[k], back.at[k], band_send.at[k], band_recv.at[k], (target, part)
        )

        @pl.when((target >= 0) & (target < bands))
        def _():
            sends[k].start()

    def slab(index):
        return pl.ds(index * rows, rows)

    fars, nears, onwards = [], [], []
    for c in range(chunks):
        source = sender_ref.at[slab(c), :]
        fars.append(
            remote(source, held.at[part, slab(c), :], far_send.at[c], far_recv.at[c], (band, across))
        )
        nears.append(
            remote(source, held.at[part, slab(c), :], near_send.at[c], near_recv.at[c], (band, beside))
        )
        fars[c].start()
        nears[c].start()
    held[part] = sender_ref[...]

    def node_row(k):
        ids = lax.broadcasted_iota(jnp.int32, (node_count, capacity), 0)
        return jnp.where(ids == wanted_ref[k : k + 1, :], 1.0, 0.0).astype(jnp.bfloat16)

    node_sum = jnp.dot(node_row(reach), slot_ref[reach], preferred_element_type=jnp.float32)
    for k in reversed(order):
        source = band + reach - k

        @pl.when((source >= 0) & (source < bands))
        def _():
            sends[k].wait_recv()

        @pl.when((source < 0) | (source >= bands))
        def _():
            back[k] = jnp.zeros((capacity, hidden), back.dtype)

        node_sum += jnp.dot(node_row(k), back[k], preferred_element_type=jnp.float32)
    node_stage[...] = node_sum.astype(node_stage.dtype)
    node_held[part] = node_sum.astype(node_held.dtype)
    fars.append(
        remote(node_stage, node_held.at[part], far_send.at[chunks], far_recv.at[chunks], (band, across))
    )
    nears.append(
        remote(node_stage, node_held.at[part], near_send.at[chunks], near_recv.at[chunks], (band, beside))
    )
    fars[chunks].start()
    nears[chunks].start()

    def pass_on(c):
        fars[c].wait_recv()
        block = held.at[across, slab(c), :] if c < chunks else node_held.at[across]
        onwards.append(remote(block, block, pass_send.at[c], pass_recv.at[c], (band, beside)))
        onwards[c].start()

    def finish(c):
        nears[c].wait_recv()
        onwards[c].wait_recv()
        if c < chunks:
            blocks = [held[j, c * rows : (c + 1) * rows, :] for j in range(held.shape[0])]
            weights = [weight_ref[0, j] for j in range(held.shape[0])]
        else:
            blocks = [node_held[j] for j in range(held.shape[0])]
            weights = [weight_ref[1, j] for j in range(held.shape[0])]
        total = lax.dot_general(
            jnp.concatenate(blocks, axis=1), jnp.concatenate(weights, axis=1), DIMS_NT,
            preferred_element_type=jnp.float32,
        )
        if c < chunks:
            grid_ref[c * rows : (c + 1) * rows, :] = total.astype(grid_ref.dtype)
        else:
            node_ref[...] = total.astype(node_ref.dtype)

    for c in range(chunks + 1):
        pass_on(c)
        if c > 0:
            finish(c - 1)
    finish(chunks)
    for c in range(chunks + 1):
        fars[c].wait_send()
        nears[c].wait_send()
        onwards[c].wait_send()
    for k in order:
        target = band + k - reach

        @pl.when((target >= 0) & (target < bands))
        def _():
            sends[k].wait_send()


def collect(slot_sum, sender_sum, wanted, weights, node_count, reach):
    span, capacity = wanted.shape
    grid_rows, hidden = sender_sum.shape
    _, parts, out_cols, _ = weights.shape
    chunks = 4
    tokens = chunks + 1
    return pl.pallas_call(
        functools.partial(collect_kernel, reach=reach, chunks=chunks),
        in_specs=[VMEM_SPEC] * 4,
        out_specs=[VMEM_SPEC] * 2,
        out_shape=[
            jax.ShapeDtypeStruct((grid_rows, out_cols), jnp.bfloat16),
            jax.ShapeDtypeStruct((node_count, out_cols), jnp.bfloat16),
        ],
        scratch_shapes=[
            pltpu.VMEM((span, capacity, hidden), jnp.bfloat16),
            pltpu.VMEM((parts, grid_rows, hidden), jnp.bfloat16),
            pltpu.VMEM((node_count, hidden), jnp.bfloat16),
            pltpu.VMEM((parts, node_count, hidden), jnp.bfloat16),
        ]
        + [DMA_SEM((span,))] * 2
        + [DMA_SEM((tokens,))] * 6,
        compiler_params=pltpu.CompilerParams(collective_id=1, has_side_effects=True),
        name="collect",
    )(slot_sum.reshape(span, capacity, hidden), sender_sum, wanted, weights)


def per_device(
    grid_latent,
    edge_latent,
    mesh_latent,
    mesh_grad,
    counts,
    request,
    edge_sender,
    edge_slot,
    w_send,
    w_recv,
    w_edge,
    edge_bias,
    w_out,
):
    span = request.shape[1]
    reach = (span - 1) // 2
    parts = lax.axis_size("mp")
    wanted = request[0]
    table, weights = spread(
        mesh_latent, mesh_grad, counts, wanted, w_recv, w_out, w_send, parts, reach
    )
    sender_sum, slot_sum = edge_pass(
        grid_latent, edge_latent, table, edge_sender, edge_slot, w_send, w_edge, edge_bias, jnp.bfloat16
    )
    return tuple(collect(slot_sum, sender_sum, wanted, weights, mesh_latent.shape[0], reach))


def solution(mesh):
    in_specs = (
        P("band", None),
        P("band", None),
        P("band", "mp"),
        P("band", "mp"),
        P("band"),
        P("band", None, None),
        P("band"),
        P("band"),
        P(None, "mp"),
        P(None, "mp"),
        P(None, "mp"),
        P("mp"),
        P("mp", None),
    )
    out_specs = (P("band", "mp"), P("band", "mp"))
    return jax.shard_map(
        per_device, mesh=mesh, in_specs=in_specs, out_specs=out_specs, check_vma=False
    )
```
